32 devices in a mesh: band: 16 (over z, y, core), fft: 2 (over x).
Axes of the slice: x: 2, y: 2, z: 4, core: 2. Of those that a mesh axis runs over, the one named last changes fastest.
Arguments:
- coefficients: float32 [16, 2, 72, 5184], P('band', None, None, 'fft'), may hold values from -0.009765625 to 0.009765625
- col_index: int32 [5184], replicated, may hold values from 0 to 5183, each once
- occupation: int32 [16], P('band'), may hold values from 1 to 4
Outputs:
- density: float32 [288, 288, 288], P('band', 'fft')
The draws below stay inside these ranges and needn't reach their ends.
Inputs may be any that keep to these rules, and one draw needn't show every extreme that they name: `col_index`: each number of the range appears once.
All inputs are finite; a program needn't handle non-finite values.
Results may differ from the reference program's by a relative error of at most 0.0003.
Values sent between devices are 32-bit elements; how exact they have to be, the bound alone decides.
A program may use at most 128 MiB of HBM per device.

```python
import jax
import jax.numpy as jnp
from jax import lax

NC = 144
NF = 288
KZ = 72
R = 36
NCOLS = 5184
BANDS = 16


def set_ends(values, rng, smallest, top_value):
    index_at = [jax.random.randint(jax.random.fold_in(rng, axis), (), 0, length) for axis, length in enumerate(values.shape)]
    widest = values.shape.index(max(values.shape))
    next_to = index_at[:widest] + [(index_at[widest] + 1) % values.shape[widest]] + index_at[widest + 1:]
    return values.at[tuple(index_at)].set(smallest).at[tuple(next_to)].set(top_value)


def block_levels(stream_key, extent, cuts, least, top_value):
    def one(dim, parts):
        steps = jax.random.uniform(jax.random.fold_in(jax.random.fold_in(stream_key, 6), dim), (parts,), jnp.float32, least / len(cuts), top_value / len(cuts))
        return jnp.repeat(jnp.exp(steps), extent[dim] // parts).reshape((-1,) + (1,) * (len(extent) - dim - 1))

    loudness = one(*cuts[0])
    for cut in cuts[1:]:
        loudness = loudness * one(*cut)
    return loudness


def noise(own_key, shape, scale, limit, shards=(), kind=jnp.bfloat16):
    entries = jax.random.normal(own_key, shape, jnp.float32) * scale
    if len(shards) > 0:
        entries = block_levels(own_key, shape, shards, -0.22, 0.18) * entries
    return jnp.clip(entries, min=-limit, max=limit).astype(kind)


def setup_inputs(seed: int = 0) -> dict:
    splits = jax.random.split(jax.random.key(seed), 4)
    return {
        "coefficients": noise(splits[0], (BANDS, 2, KZ, NCOLS), (8 * R**3) ** -0.5, 0.009765625, ((0, 16), (3, 2)), jnp.float32),
        "col_index": jax.random.permutation(splits[1], NCOLS).astype(jnp.int32),
        "occupation": set_ends(jax.random.randint(splits[2], (BANDS,), 1, 5), jax.random.fold_in(splits[2], 1), 1, 4).astype(jnp.int32),
    }


def sphere_mask(radius, side_len):
    wave_index = jnp.arange(side_len, dtype=jnp.int32) - radius
    square = wave_index * wave_index
    total_sq = square[:, None, None] + square[None, :, None] + square[None, None, :]
    return (total_sq <= radius * radius).astype(jnp.float32)


def reference(coefficients, col_index, occupation):
    inverse = jnp.zeros((NCOLS,), jnp.int32).at[col_index].set(jnp.arange(NCOLS, dtype=jnp.int32))
    inside = sphere_mask(R, KZ)

    def add_band(band_index, summed):
        box_grid = jnp.take(coefficients[band_index], inverse, axis=2).reshape(2, KZ, KZ, KZ)
        box_grid = jnp.transpose(box_grid, (0, 2, 3, 1)) * inside
        spectrum = lax.complex(box_grid[0], box_grid[1])
        padded = jnp.zeros((NC, NC, NC), spectrum.dtype).at[:KZ, :KZ, :KZ].set(spectrum)
        padded = jnp.roll(padded, (-R, -R, -R), axis=(0, 1, 2))
        wave_field = jnp.fft.ifftn(padded) * float(NC * NC * NC)
        real_part = jnp.real(wave_field)
        imag_part = jnp.imag(wave_field)
        moduli = real_part * real_part + imag_part * imag_part
        return summed + occupation[band_index].astype(jnp.float32) * moduli

    coarse_density = lax.fori_loop(0, BANDS, add_band, jnp.zeros((NC, NC, NC), jnp.float32)) / BANDS
    spectrum = jnp.fft.fftn(coarse_density) / float(NC * NC * NC)
    kept_mask = (jnp.arange(NC, dtype=jnp.int32) != NC // 2).astype(jnp.float32)
    spectrum = spectrum * (kept_mask[:, None, None] * kept_mask[None, :, None] * kept_mask[None, None, :])
    target = jnp.arange(NC, dtype=jnp.int32)
    target = jnp.where(target < NC // 2, target, target + NF - NC)
    fine_spec = jnp.zeros((NF, NF, NF), spectrum.dtype)
    fine_spec = fine_spec.at[target[:, None, None], target[None, :, None], target[None, None, :]].set(spectrum)
    density = jnp.real(jnp.fft.ifftn(fine_spec)) * float(NF * NF * NF)
    return density.astype(jnp.float32)
```

```python
import math

import jax
import jax.numpy as jnp
import numpy as np
from jax import lax
from jax.experimental import pallas as pl
from jax.experimental.pallas import tpu as pltpu
from jax.sharding import PartitionSpec as P

NC = 144
NF = 288
KZ = 72
NCOLS = KZ * KZ
LANES = 128
MESH = pl.DeviceIdType.MESH


def product(pattern, operand_a, operand_b):
    return jnp.einsum(pattern, operand_a, operand_b, precision=lax.Precision.HIGH)


def round_up(size, unit):
    return -(-size // unit) * unit


def phase_tables():
    wave = np.arange(KZ) - KZ // 2
    angles = np.mod(np.arange(NC)[:, None] * wave[None, :], NC) * (2.0 * math.pi / NC)
    return np.cos(angles), np.sin(angles)


def interpolation_matrix():
    offsets = np.arange(NF)[:, None] - 2 * np.arange(NC)[None, :]
    waves = np.arange(1, NC // 2)
    angles = np.mod(offsets[:, :, None] * waves, NF) * (2.0 * math.pi / NF)
    return ((1.0 + 2.0 * np.sum(np.cos(angles), axis=2)) / NC).astype(np.float32)


def line_table(planes_padded):
    cos_t, sin_t = phase_tables()
    table = np.zeros((planes_padded, 2, 2, KZ), np.float32)
    table[:NC, 0, 0], table[:NC, 0, 1] = cos_t, -sin_t
    table[:NC, 1, 0], table[:NC, 1, 1] = sin_t, cos_t
    return table


def split_table():
    cos_t, sin_t = phase_tables()
    table = np.concatenate([cos_t, sin_t], axis=0).astype(np.float32)
    high = table.astype(jnp.bfloat16)
    low = (table - high.astype(np.float32)).astype(jnp.bfloat16)
    return np.concatenate([high, high, low], axis=1)


def exchange_kernel(src, dst, send_sem, recv_sem, local_sem):
    fft_size = lax.axis_size("fft")
    total = lax.axis_size("band") * fft_size
    me = lax.axis_index("band") * fft_size + lax.axis_index("fft")
    barrier = pltpu.get_barrier_semaphore()
    targets = []
    for step in range(1, total):
        target = lax.rem(me + step, total)
        targets.append((target, (target // fft_size, lax.rem(target, fft_size))))
        pl.semaphore_signal(barrier, inc=1, device_id=targets[-1][1], device_id_type=MESH)
    own = pltpu.make_async_copy(src.at[me], dst.at[me], local_sem)
    own.start()
    pl.semaphore_wait(barrier, total - 1)
    copies = []
    for step in range(1, total):
        target, device = targets[step - 1]
        copy = pltpu.make_async_remote_copy(
            src_ref=src.at[target],
            dst_ref=dst.at[me],
            send_sem=send_sem.at[step],
            recv_sem=recv_sem.at[step],
            device_id=device,
            device_id_type=MESH,
        )
        copy.start()
        copies.append(copy)
    own.wait()
    for copy in copies:
        copy.wait()


def exchange(blocks, collective_id):
    total = blocks.shape[0]
    return pl.pallas_call(
        exchange_kernel,
        out_shape=jax.ShapeDtypeStruct(blocks.shape, blocks.dtype),
        in_specs=[pl.BlockSpec(memory_space=pl.ANY)],
        out_specs=pl.BlockSpec(memory_space=pl.ANY),
        scratch_shapes=[
            pltpu.SemaphoreType.DMA((total,)),
            pltpu.SemaphoreType.DMA((total,)),
            pltpu.SemaphoreType.DMA,
        ],
        compiler_params=pltpu.CompilerParams(collective_id=collective_id, has_side_effects=True),
        name=f"exchange{collective_id}",
    )(blocks)


def split_rows(data):
    high = data.astype(jnp.bfloat16).astype(jnp.float32)
    return jnp.concatenate([high, data - high, high], axis=0).astype(jnp.bfloat16)


def plane_kernel(cols, columns, index, table, pick, out, rows, box, half_re, half_im):
    parts, _, lanes, cols_padded = columns.shape
    for part in range(parts):
        def turn(block, carry):
            at = pl.multiple_of(block * LANES, LANES)
            for which in range(2):
                rows[pl.ds(part * cols_padded + at, LANES), pl.ds(which * lanes, lanes)] = columns[
                    part, which, :, pl.ds(at, LANES)
                ].T
            return carry

        lax.fori_loop(0, cols_padded // LANES, turn, 0)

    unroll = math.gcd(cols, 8)
    for part in range(parts):
        def place(step, carry):
            for lane in range(unroll):
                col = step * unroll + lane
                box[pl.ds(index[part * cols + col], 1), :] = rows[
                    pl.ds(part * cols_padded + col, 1), :
                ]
            return carry

        lax.fori_loop(0, cols // unroll, place, 0)

    def rotate(stacked):
        full = jnp.dot(table[...], stacked, preferred_element_type=jnp.float32)
        real = full[:NC, :lanes] - full[NC:, lanes:]
        imag = full[NC:, :lanes] + full[:NC, lanes:]
        return real, imag

    def second(first, carry):
        data = box[pl.ds(pl.multiple_of(first * KZ, 8), KZ), :]
        real, imag = rotate(split_rows(data))
        at = pl.ds(pl.multiple_of(first * NC, 8), NC)
        half_re[at, :] = real
        half_im[at, :] = imag
        return carry

    lax.fori_loop(0, KZ, second, 0)

    def third(point, carry):
        at = pl.ds(point, KZ, stride=NC)
        data = jnp.concatenate([half_re[at, :], half_im[at, :]], axis=1)
        real, imag = rotate(split_rows(data))
        moduli = real * real + imag * imag
        high = moduli.astype(jnp.bfloat16)
        low = (moduli - high.astype(jnp.float32)).astype(jnp.bfloat16)
        both = jnp.concatenate([high, low], axis=1)
        out[point] = lax.dot_general(
            pick[...], both, (((1,), (1,)), ((), ())), preferred_element_type=jnp.float32
        )
        return carry

    lax.fori_loop(0, NC, third, 0)


def local(coefficients, col_index, occupation):
    band_here, _, _, cols = coefficients.shape
    band_size, fft_size = lax.axis_size("band"), lax.axis_size("fft")
    total = band_size * fft_size
    bands = band_here * band_size
    planes = -(-NC // total)
    radius = KZ // 2
    local_cols = lax.dynamic_slice_in_dim(col_index, lax.axis_index("fft") * cols, cols)
    first_wave = local_cols // KZ - radius
    second_wave = local_cols % KZ - radius
    third_wave = jnp.arange(KZ, dtype=jnp.int32) - radius
    radial = (first_wave * first_wave + second_wave * second_wave)[None, :] + (
        third_wave * third_wave
    )[:, None]
    inside = (radial <= radius * radius).astype(jnp.float32)
    amplitude = jnp.sqrt(occupation.astype(jnp.float32) / bands)
    masked = coefficients * inside * amplitude[:, None, None, None]

    table = jnp.asarray(line_table(total * planes))
    lines = product("zpqk,bqkc->zbpc", table, masked)
    lines = lines.reshape(total, planes * band_here, 2, cols)
    lines = exchange(lines, 0)

    columns = lines.reshape(band_size, fft_size, planes * band_here, 2, cols)
    columns = columns.transpose(1, 3, 0, 2, 4).reshape(fft_size, 2, band_size * planes * band_here, cols)
    lane_count = band_size * planes * band_here
    lanes = round_up(lane_count, LANES)
    cols_padded = round_up(cols, LANES)
    columns = jnp.pad(columns, ((0, 0), (0, 0), (0, lanes - lane_count), (0, cols_padded - cols)))

    plane_rows = round_up(planes, 8)
    pick = np.zeros((plane_rows, lanes), np.float32)
    lane = np.arange(lane_count)
    pick[(lane // band_here) % planes, lane] = 1.0
    pick = jnp.asarray(np.concatenate([pick, pick], axis=1), jnp.bfloat16)

    vmem = pl.BlockSpec(memory_space=pltpu.VMEM)
    density = pl.pallas_call(
        lambda *refs: plane_kernel(cols, *refs),
        out_shape=jax.ShapeDtypeStruct((NC, plane_rows, NC), jnp.float32),
        in_specs=[vmem, pl.BlockSpec(memory_space=pltpu.SMEM), vmem, vmem],
        out_specs=vmem,
        scratch_shapes=[
            pltpu.VMEM((fft_size * cols_padded, 2 * lanes), jnp.float32),
            pltpu.VMEM((NCOLS, 2 * lanes), jnp.float32),
            pltpu.VMEM((KZ * NC, lanes), jnp.float32),
            pltpu.VMEM((KZ * NC, lanes), jnp.float32),
        ],
        compiler_params=pltpu.CompilerParams(vmem_limit_bytes=56 * 1024 * 1024),
        name="planes",
    )(columns, col_index, jnp.asarray(split_table()), pick)

    interpolation = jnp.asarray(interpolation_matrix())
    row_share = NF // band_size
    wide = product("ga,bza->gzb", interpolation, density[:, :planes])
    chunk = row_share * planes * NC
    chunk_padded = round_up(chunk, 8 * LANES)
    wide = jnp.pad(wide.reshape(band_size, chunk), ((0, 0), (0, chunk_padded - chunk)))
    wide = wide.reshape(band_size, 1, chunk_padded // LANES, LANES)
    wide = jnp.broadcast_to(wide, (band_size, fft_size) + wide.shape[2:])
    wide = exchange(wide.reshape(total, chunk_padded // LANES, LANES), 1)
    wide = wide.reshape(total, chunk_padded)[:, :chunk].reshape(total, row_share, planes, NC)

    col_share = NF // fft_size
    own = lax.dynamic_slice_in_dim(interpolation, lax.axis_index("fft") * col_share, col_share, 0)
    full = product("tgpb,fb->gftp", wide, own).reshape(row_share, col_share, total * planes)
    last = jnp.asarray(np.pad(interpolation_matrix(), ((0, 0), (0, total * planes - NC))))
    return product("gfz,hz->gfh", full, last)


def solution(mesh):
    return jax.shard_map(
        local,
        mesh=mesh,
        in_specs=(P("band", None, None, "fft"), P(), P("band")),
        out_specs=P("band", "fft", None),
        check_vma=False,
    )
```

```python
import math

import jax
import jax.numpy as jnp
import numpy as np
from jax import lax
from jax.experimental import pallas as pl
from jax.experimental.pallas import tpu as pltpu
from jax.sharding import PartitionSpec as P

NC = 144
NF = 288
KZ = 72
NCOLS = KZ * KZ
LANES = 128
FOLD_WAVES = 40
FOLD_POINTS = 80
MESH = pl.DeviceIdType.MESH


def product(pattern, operand_a, operand_b):
    return jnp.einsum(pattern, operand_a, operand_b, precision=lax.Precision.HIGH)


def round_up(size, unit):
    return -(-size // unit) * unit


def phase_tables():
    wave = np.arange(KZ) - KZ // 2
    angles = np.mod(np.arange(NC)[:, None] * wave[None, :], NC) * (2.0 * math.pi / NC)
    return np.cos(angles), np.sin(angles)


def interpolation_matrix():
    offsets = np.arange(NF)[:, None] - 2 * np.arange(NC)[None, :]
    waves = np.arange(1, NC // 2)
    angles = np.mod(offsets[:, :, None] * waves, NF) * (2.0 * math.pi / NF)
    return ((1.0 + 2.0 * np.sum(np.cos(angles), axis=2)) / NC).astype(np.float32)


def line_table(planes_padded):
    cos_t, sin_t = phase_tables()
    table = np.zeros((planes_padded, 2, 2, KZ), np.float32)
    table[:NC, 0, 0], table[:NC, 0, 1] = cos_t, -sin_t
    table[:NC, 1, 0], table[:NC, 1, 1] = sin_t, cos_t
    return table


def fold_tables():
    half = KZ // 2
    points = np.arange(NC // 2 + 1)
    waves = np.concatenate([np.arange(half), [half]])
    angles = np.mod(points[:, None] * waves[None, :], NC) * (2.0 * math.pi / NC)
    tables = []
    for values in (np.cos(angles), np.sin(angles)):
        table = np.zeros((FOLD_POINTS, FOLD_WAVES), np.float32)
        table[: NC // 2 + 1, : half + 1] = values
        high = table.astype(jnp.bfloat16)
        low = (table - high.astype(np.float32)).astype(jnp.bfloat16)
        tables.append(np.concatenate([high, high, low], axis=1))
    return np.stack(tables)


def fold_slots():
    points = np.arange(NC)
    return np.where(points <= NC // 2, points, FOLD_POINTS + NC - points)


def wave_slots(index):
    half = KZ // 2
    return jnp.where(index >= half, index - half, jnp.where(index == 0, half, KZ - index))


def exchange_kernel(src, dst, send_sem, recv_sem, local_sem):
    fft_size = lax.axis_size("fft")
    total = lax.axis_size("band") * fft_size
    me = lax.axis_index("band") * fft_size + lax.axis_index("fft")
    barrier = pltpu.get_barrier_semaphore()
    targets = []
    for step in range(1, total):
        target = lax.rem(me + step, total)
        targets.append((target, (target // fft_size, lax.rem(target, fft_size))))
        pl.semaphore_signal(barrier, inc=1, device_id=targets[-1][1], device_id_type=MESH)
    own = pltpu.make_async_copy(src.at[me], dst.at[me], local_sem)
    own.start()
    pl.semaphore_wait(barrier, total - 1)
    copies = []
    for step in range(1, total):
        target, device = targets[step - 1]
        copy = pltpu.make_async_remote_copy(
            src_ref=src.at[target],
            dst_ref=dst.at[me],
            send_sem=send_sem.at[step],
            recv_sem=recv_sem.at[step],
            device_id=device,
            device_id_type=MESH,
        )
        copy.start()
        copies.append(copy)
    own.wait()
    for copy in copies:
        copy.wait()


def exchange(blocks, collective_id):
    total = blocks.shape[0]
    return pl.pallas_call(
        exchange_kernel,
        out_shape=jax.ShapeDtypeStruct(blocks.shape, blocks.dtype),
        in_specs=[pl.BlockSpec(memory_space=pl.ANY)],
        out_specs=pl.BlockSpec(memory_space=pl.ANY),
        scratch_shapes=[
            pltpu.SemaphoreType.DMA((total,)),
            pltpu.SemaphoreType.DMA((total,)),
            pltpu.SemaphoreType.DMA,
        ],
        compiler_params=pltpu.CompilerParams(collective_id=collective_id, has_side_effects=True),
        name=f"exchange{collective_id}",
    )(blocks)


def split_rows(data):
    high = data.astype(jnp.bfloat16).astype(jnp.float32)
    return jnp.concatenate([high, data - high, high], axis=0).astype(jnp.bfloat16)


def plane_kernel(cols, columns, index, table, pick, out, rows, box, half_re, half_im):
    parts, _, lanes, cols_padded = columns.shape
    for part in range(parts):
        def turn(block, carry):
            at = pl.multiple_of(block * LANES, LANES)
            for which in range(2):
                rows[pl.ds(part * cols_padded + at, LANES), pl.ds(which * lanes, lanes)] = columns[
                    part, which, :, pl.ds(at, LANES)
                ].T
            return carry

        lax.fori_loop(0, cols_padded // LANES, turn, 0)

    unroll = math.gcd(cols, 8)
    for part in range(parts):
        def place(step, carry):
            for lane in range(unroll):
                col = step * unroll + lane
                box[pl.ds(index[part * cols + col], 1), :] = rows[
                    pl.ds(part * cols_padded + col, 1), :
                ]
            return carry

        lax.fori_loop(0, cols // unroll, place, 0)

    half = KZ // 2
    single = lax.broadcasted_iota(jnp.int32, (half + 4, 2 * lanes), 0)[:half] == 0
    last_row = lax.broadcasted_iota(jnp.int32, (8, 2 * lanes), 0)[: FOLD_WAVES - half] == 0

    def rotate(ahead, behind):
        alone = jnp.where(last_row, jnp.broadcast_to(behind[:1], last_row.shape), 0.0)
        behind = jnp.where(single, 0.0, behind)
        even = jnp.concatenate([ahead + behind, alone], axis=0)
        odd = jnp.concatenate([ahead - behind, -alone], axis=0)
        cos_part = jnp.dot(table[0], split_rows(even), preferred_element_type=jnp.float32)
        sin_part = jnp.dot(table[1], split_rows(odd), preferred_element_type=jnp.float32)
        cos_re, cos_im = cos_part[:, :lanes], cos_part[:, lanes:]
        sin_re, sin_im = sin_part[:, :lanes], sin_part[:, lanes:]
        real = jnp.concatenate([cos_re - sin_im, cos_re + sin_im], axis=0)
        imag = jnp.concatenate([cos_im + sin_re, cos_im - sin_re], axis=0)
        return real, imag

    slots = 2 * FOLD_POINTS

    def second(first, carry):
        at = pl.multiple_of(first * KZ, 8)
        data = box[pl.ds(at, KZ), :]
        real, imag = rotate(data[:half], data[half:])
        at = pl.ds(pl.multiple_of(first * slots, 8), slots)
        half_re[at, :] = real
        half_im[at, :] = imag
        return carry

    lax.fori_loop(0, KZ, second, 0, unroll=4)

    def third(point, carry):
        slot = jnp.where(point <= NC // 2, point, point + FOLD_POINTS - NC // 2)
        parts = []
        for base in (0, half):
            at = pl.ds(slot + base * slots, half, stride=slots)
            parts.append(jnp.concatenate([half_re[at, :], half_im[at, :]], axis=1))
        real, imag = rotate(*parts)
        moduli = real * real + imag * imag
        high = moduli.astype(jnp.bfloat16)
        low = (moduli - high.astype(jnp.float32)).astype(jnp.bfloat16)
        both = jnp.concatenate([high, low], axis=1)
        out[point] = lax.dot_general(
            pick[...], both, (((1,), (1,)), ((), ())), preferred_element_type=jnp.float32
        )
        return carry

    lax.fori_loop(0, NC, third, 0, unroll=4)


def local(coefficients, col_index, occupation):
    band_here, _, _, cols = coefficients.shape
    band_size, fft_size = lax.axis_size("band"), lax.axis_size("fft")
    total = band_size * fft_size
    bands = band_here * band_size
    planes = -(-NC // total)
    radius = KZ // 2
    local_cols = lax.dynamic_slice_in_dim(col_index, lax.axis_index("fft") * cols, cols)
    first_wave = local_cols // KZ - radius
    second_wave = local_cols % KZ - radius
    third_wave = jnp.arange(KZ, dtype=jnp.int32) - radius
    radial = (first_wave * first_wave + second_wave * second_wave)[None, :] + (
        third_wave * third_wave
    )[:, None]
    inside = (radial <= radius * radius).astype(jnp.float32)
    amplitude = jnp.sqrt(occupation.astype(jnp.float32) / bands)
    masked = coefficients * inside * amplitude[:, None, None, None]

    table = jnp.asarray(line_table(total * planes))
    lines = product("zpqk,bqkc->zbpc", table, masked)
    lines = lines.reshape(total, planes * band_here, 2, cols)
    lines = exchange(lines, 0)

    columns = lines.reshape(band_size, fft_size, planes * band_here, 2, cols)
    columns = columns.transpose(1, 3, 0, 2, 4).reshape(fft_size, 2, band_size * planes * band_here, cols)
    lane_count = band_size * planes * band_here
    lanes = round_up(lane_count, LANES)
    cols_padded = round_up(cols, LANES)
    columns = jnp.pad(columns, ((0, 0), (0, 0), (0, lanes - lane_count), (0, cols_padded - cols)))

    plane_rows = round_up(planes, 8)
    pick = np.zeros((plane_rows, lanes), np.float32)
    lane = np.arange(lane_count)
    pick[(lane // band_here) % planes, lane] = 1.0
    pick = jnp.asarray(np.concatenate([pick, pick], axis=1), jnp.bfloat16)

    places = wave_slots(col_index // KZ) * KZ + wave_slots(col_index % KZ)
    vmem = pl.BlockSpec(memory_space=pltpu.VMEM)
    density = pl.pallas_call(
        lambda *refs: plane_kernel(cols, *refs),
        out_shape=jax.ShapeDtypeStruct((NC, plane_rows, 2 * FOLD_POINTS), jnp.float32),
        in_specs=[vmem, pl.BlockSpec(memory_space=pltpu.SMEM), vmem, vmem],
        out_specs=vmem,
        scratch_shapes=[
            pltpu.VMEM((fft_size * cols_padded, 2 * lanes), jnp.float32),
            pltpu.VMEM((NCOLS, 2 * lanes), jnp.float32),
            pltpu.VMEM((KZ * 2 * FOLD_POINTS, lanes), jnp.float32),
            pltpu.VMEM((KZ * 2 * FOLD_POINTS, lanes), jnp.float32),
        ],
        compiler_params=pltpu.CompilerParams(vmem_limit_bytes=56 * 1024 * 1024),
        name="planes",
    )(columns, places, jnp.asarray(fold_tables()), pick)

    row_share = NF // band_size
    first_table = np.zeros((NF, 2 * FOLD_POINTS), np.float32)
    first_table[:, fold_slots()] = interpolation_matrix()
    wide = product("ga,bza->gzb", jnp.asarray(first_table), density[:, :planes])
    chunk = row_share * planes * NC
    chunk_padded = round_up(chunk, 8 * LANES)
    wide = jnp.pad(wide.reshape(band_size, chunk), ((0, 0), (0, chunk_padded - chunk)))
    wide = wide.reshape(band_size, 1, chunk_padded // LANES, LANES)
    wide = jnp.broadcast_to(wide, (band_size, fft_size) + wide.shape[2:])
    wide = exchange(wide.reshape(total, chunk_padded // LANES, LANES), 1)
    wide = wide.reshape(total, chunk_padded)[:, :chunk].reshape(total, row_share, planes, NC)

    col_share = NF // fft_size
    order = np.concatenate([np.arange(NC // 2 + 1), np.arange(NC - 1, NC // 2, -1)])
    interpolation = jnp.asarray(interpolation_matrix()[:, order])
    own = lax.dynamic_slice_in_dim(interpolation, lax.axis_index("fft") * col_share, col_share, 0)
    full = product("tgpb,fb->gftp", wide, own).reshape(row_share, col_share, total * planes)
    last = jnp.asarray(np.pad(interpolation_matrix(), ((0, 0), (0, total * planes - NC))))
    return product("gfz,hz->gfh", full, last)


def solution(mesh):
    return jax.shard_map(
        local,
        mesh=mesh,
        in_specs=(P("band", None, None, "fft"), P(), P("band")),
        out_specs=P("band", "fft", None),
        check_vma=False,
    )
```

```python
import math

import jax
import jax.numpy as jnp
import numpy as np
from jax import lax
from jax.experimental import pallas as pl
from jax.experimental.pallas import tpu as pltpu
from jax.sharding import PartitionSpec as P

NC = 144
NF = 288
KZ = 72
NCOLS = KZ * KZ
LANES = 128
LAYERS = 4
FOLD_WAVES = 40
FOLD_POINTS = 80
MESH = pl.DeviceIdType.MESH


def product(pattern, operand_a, operand_b):
    return jnp.einsum(pattern, operand_a, operand_b, precision=lax.Precision.HIGH)


def round_up(size, unit):
    return -(-size // unit) * unit


def phase_tables():
    wave = np.arange(KZ) - KZ // 2
    angles = np.mod(np.arange(NC)[:, None] * wave[None, :], NC) * (2.0 * math.pi / NC)
    return np.cos(angles), np.sin(angles)


def interpolation_matrix():
    offsets = np.arange(NF)[:, None] - 2 * np.arange(NC)[None, :]
    waves = np.arange(1, NC // 2)
    angles = np.mod(offsets[:, :, None] * waves, NF) * (2.0 * math.pi / NF)
    return ((1.0 + 2.0 * np.sum(np.cos(angles), axis=2)) / NC).astype(np.float32)


def line_table(planes_padded):
    cos_t, sin_t = phase_tables()
    table = np.zeros((planes_padded, 2, 2, KZ), np.float32)
    table[:NC, 0, 0], table[:NC, 0, 1] = cos_t, -sin_t
    table[:NC, 1, 0], table[:NC, 1, 1] = sin_t, cos_t
    return table


def fold_tables():
    half = KZ // 2
    points = np.arange(NC // 2 + 1)
    waves = np.concatenate([np.arange(half), [half]])
    angles = np.mod(points[:, None] * waves[None, :], NC) * (2.0 * math.pi / NC)
    tables = []
    for values in (np.cos(angles), np.sin(angles)):
        table = np.zeros((FOLD_POINTS, FOLD_WAVES), np.float32)
        table[: NC // 2 + 1, : half + 1] = values
        high = table.astype(jnp.bfloat16)
        low = (table - high.astype(np.float32)).astype(jnp.bfloat16)
        tables.append(np.concatenate([high, high, low], axis=1))
    return np.stack(tables)


def wave_slots(index):
    half = KZ // 2
    return jnp.where(index >= half, index - half, jnp.where(index == 0, half, KZ - index))


def exchange_kernel(scope, src, dst, send_sem, recv_sem, local_sem):
    band_size, fft_size = lax.axis_size("band"), lax.axis_size("fft")
    band, fft = lax.axis_index("band"), lax.axis_index("fft")
    layer = band_size // LAYERS
    if scope == "all":
        total, me = band_size * fft_size, band * fft_size + fft
    elif scope == "layer":
        total, me = layer * fft_size, lax.rem(band, layer) * fft_size + fft
    else:
        total, me = LAYERS, band // layer

    def device_of(target):
        if scope == "all":
            return (target // fft_size, lax.rem(target, fft_size))
        if scope == "layer":
            return (band // layer * layer + target // fft_size, lax.rem(target, fft_size))
        return (target * layer + lax.rem(band, layer), fft)

    barrier = pltpu.get_barrier_semaphore()
    targets = []
    for step in range(1, total):
        target = lax.rem(me + step, total)
        targets.append((target, device_of(target)))
        pl.semaphore_signal(barrier, inc=1, device_id=targets[-1][1], device_id_type=MESH)
    own = pltpu.make_async_copy(src.at[me], dst.at[me], local_sem)
    own.start()
    pl.semaphore_wait(barrier, total - 1)
    copies = []
    for step in range(1, total):
        target, device = targets[step - 1]
        copy = pltpu.make_async_remote_copy(
            src_ref=src.at[target],
            dst_ref=dst.at[me],
            send_sem=send_sem.at[step],
            recv_sem=recv_sem.at[step],
            device_id=device,
            device_id_type=MESH,
        )
        copy.start()
        copies.append(copy)
    own.wait()
    for copy in copies:
        copy.wait()


def exchange(blocks, scope, collective_id):
    total = blocks.shape[0]
    return pl.pallas_call(
        lambda *refs: exchange_kernel(scope, *refs),
        out_shape=jax.ShapeDtypeStruct(blocks.shape, blocks.dtype),
        in_specs=[pl.BlockSpec(memory_space=pl.ANY)],
        out_specs=pl.BlockSpec(memory_space=pl.ANY),
        scratch_shapes=[
            pltpu.SemaphoreType.DMA((total,)),
            pltpu.SemaphoreType.DMA((total,)),
            pltpu.SemaphoreType.DMA,
        ],
        compiler_params=pltpu.CompilerParams(collective_id=collective_id, has_side_effects=True),
        name=f"exchange_{scope}",
    )(blocks)


def split_rows(data):
    high = data.astype(jnp.bfloat16).astype(jnp.float32)
    return jnp.concatenate([high, data - high, high], axis=0).astype(jnp.bfloat16)


def plane_kernel(cols, columns, index, table, pick, out, rows, box, half_re, half_im):
    parts, _, lanes, cols_padded = columns.shape
    for part in range(parts):
        def turn(block, carry):
            at = pl.multiple_of(block * LANES, LANES)
            for which in range(2):
                rows[pl.ds(part * cols_padded + at, LANES), pl.ds(which * lanes, lanes)] = columns[
                    part, which, :, pl.ds(at, LANES)
                ].T
            return carry

        lax.fori_loop(0, cols_padded // LANES, turn, 0)

    unroll = math.gcd(cols, 16)
    for part in range(parts):
        def place(step, carry):
            first = step * unroll
            batch = [rows[pl.ds(part * cols_padded + first + n, 1), :] for n in range(unroll)]
            to = [index[part * cols + first + n] for n in range(unroll)]
            for row, value in zip(to, batch):
                box[pl.ds(row, 1), :] = value
            return carry

        lax.fori_loop(0, cols // unroll, place, 0)

    half = KZ // 2
    single = lax.broadcasted_iota(jnp.int32, (half + 4, 2 * lanes), 0)[:half] == 0
    last_row = lax.broadcasted_iota(jnp.int32, (8, 2 * lanes), 0)[: FOLD_WAVES - half] == 0

    def rotate(ahead, behind):
        alone = jnp.where(last_row, jnp.broadcast_to(behind[:1], last_row.shape), 0.0)
        behind = jnp.where(single, 0.0, behind)
        even = jnp.concatenate([ahead + behind, alone], axis=0)
        odd = jnp.concatenate([ahead - behind, -alone], axis=0)
        cos_part = jnp.dot(table[0], split_rows(even), preferred_element_type=jnp.float32)
        sin_part = jnp.dot(table[1], split_rows(odd), preferred_element_type=jnp.float32)
        cos_re, cos_im = cos_part[:, :lanes], cos_part[:, lanes:]
        sin_re, sin_im = sin_part[:, :lanes], sin_part[:, lanes:]
        real = jnp.concatenate([cos_re - sin_im, cos_re + sin_im], axis=0)
        imag = jnp.concatenate([cos_im + sin_re, cos_im - sin_re], axis=0)
        return real, imag

    slots = 2 * FOLD_POINTS

    def second(first, carry):
        at = pl.multiple_of(first * KZ, 8)
        data = box[pl.ds(at, KZ), :]
        real, imag = rotate(data[:half], data[half:])
        at = pl.ds(pl.multiple_of(first * slots, 8), slots)
        half_re[at, :] = real
        half_im[at, :] = imag
        return carry

    lax.fori_loop(0, KZ, second, 0, unroll=4)

    def third(point, carry):
        slot = jnp.where(point <= NC // 2, point, point + FOLD_POINTS - NC // 2)
        parts = []
        for base in (0, half):
            at = pl.ds(slot + base * slots, half, stride=slots)
            parts.append(jnp.concatenate([half_re[at, :], half_im[at, :]], axis=1))
        real, imag = rotate(*parts)
        moduli = real * real + imag * imag
        high = moduli.astype(jnp.bfloat16)
        low = (moduli - high.astype(jnp.float32)).astype(jnp.bfloat16)
        both = jnp.concatenate([high, low], axis=1)
        out[point] = lax.dot_general(
            pick[...], both, (((1,), (1,)), ((), ())), preferred_element_type=jnp.float32
        )
        return carry

    lax.fori_loop(0, NC, third, 0, unroll=4)


def local(coefficients, col_index, occupation):
    band_here, _, _, cols = coefficients.shape
    band_size, fft_size = lax.axis_size("band"), lax.axis_size("fft")
    total = band_size * fft_size
    bands = band_here * band_size
    layer = band_size // LAYERS
    group = layer * fft_size
    planes = -(-NC // group)
    radius = KZ // 2
    local_cols = lax.dynamic_slice_in_dim(col_index, lax.axis_index("fft") * cols, cols)
    first_wave = local_cols // KZ - radius
    second_wave = local_cols % KZ - radius
    third_wave = jnp.arange(KZ, dtype=jnp.int32) - radius
    radial = (first_wave * first_wave + second_wave * second_wave)[None, :] + (
        third_wave * third_wave
    )[:, None]
    inside = (radial <= radius * radius).astype(jnp.float32)
    amplitude = jnp.sqrt(occupation.astype(jnp.float32) / bands)
    masked = coefficients * inside * amplitude[:, None, None, None]

    table = jnp.asarray(line_table(group * planes))
    lines = product("zpqk,bqkc->zbpc", table, masked)
    lines = lines.reshape(group, planes * band_here, 2, cols)
    lines = exchange(lines, "layer", 0)

    columns = lines.reshape(layer, fft_size, planes * band_here, 2, cols)
    columns = columns.transpose(1, 3, 0, 2, 4).reshape(fft_size, 2, layer * planes * band_here, cols)
    lane_count = layer * planes * band_here
    lanes = round_up(lane_count, LANES)
    cols_padded = round_up(cols, LANES)
    columns = jnp.pad(columns, ((0, 0), (0, 0), (0, lanes - lane_count), (0, cols_padded - cols)))

    plane_rows = round_up(planes, 8)
    pick = np.zeros((plane_rows, lanes), np.float32)
    lane = np.arange(lane_count)
    pick[(lane // band_here) % planes, lane] = 1.0
    pick = jnp.asarray(np.concatenate([pick, pick], axis=1), jnp.bfloat16)

    places = wave_slots(col_index // KZ) * KZ + wave_slots(col_index % KZ)
    vmem = pl.BlockSpec(memory_space=pltpu.VMEM)
    density = pl.pallas_call(
        lambda *refs: plane_kernel(cols, *refs),
        out_shape=jax.ShapeDtypeStruct((NC, plane_rows, 2 * FOLD_POINTS), jnp.float32),
        in_specs=[vmem, pl.BlockSpec(memory_space=pltpu.SMEM), vmem, vmem],
        out_specs=vmem,
        scratch_shapes=[
            pltpu.VMEM((fft_size * cols_padded, 2 * lanes), jnp.float32),
            pltpu.VMEM((NCOLS, 2 * lanes), jnp.float32),
            pltpu.VMEM((KZ * 2 * FOLD_POINTS, lanes), jnp.float32),
            pltpu.VMEM((KZ * 2 * FOLD_POINTS, lanes), jnp.float32),
        ],
        compiler_params=pltpu.CompilerParams(vmem_limit_bytes=56 * 1024 * 1024),
        name="planes",
    )(columns, places, jnp.asarray(fold_tables()), pick)

    row_share = NF // band_size
    kept = NC // 2 + 1
    density = density[:, :planes]
    density = jnp.concatenate(
        [density[..., :kept], density[..., FOLD_POINTS + 1 : FOLD_POINTS + 1 + NC - kept]], axis=2
    )
    points = NC // LAYERS

    def exchange_flat(blocks, chunk, scope, collective_id):
        padded = round_up(chunk, LANES)
        flat = jnp.pad(blocks.reshape(-1, chunk), ((0, 0), (0, padded - chunk)))
        flat = flat.reshape(-1, padded // LANES, LANES)
        if scope == "all":
            flat = jnp.broadcast_to(flat[:, None], (band_size, fft_size) + flat.shape[1:])
            flat = flat.reshape((total,) + flat.shape[2:])
        return exchange(flat, scope, collective_id)

    part = exchange_flat(density, points * planes * NC, "column", 1)
    summed = jnp.sum(part, axis=0).reshape(-1)[: points * planes * NC]
    summed = summed.reshape(points, planes, NC)

    order = np.concatenate([np.arange(kept), np.arange(NC - 1, kept - 1, -1)])
    interpolation = jnp.asarray(interpolation_matrix()[:, order])
    row_share = NF // band_size
    wide = product("ga,pza->gzp", interpolation, summed)
    chunk = row_share * planes * points
    wide = exchange_flat(wide, chunk, "all", 2)
    wide = wide.reshape(total, -1)[:, :chunk].reshape(LAYERS, group, row_share, planes, points)

    col_share = NF // fft_size
    own = lax.dynamic_slice_in_dim(interpolation, lax.axis_index("fft") * col_share, col_share, 0)
    wide = wide.transpose(2, 1, 3, 0, 4).reshape(row_share, group * planes, NC)
    full = product("gzb,fb->gfz", wide, own)
    last = jnp.asarray(np.pad(interpolation_matrix(), ((0, 0), (0, group * planes - NC))))
    return product("gfz,hz->gfh", full, last)


def solution(mesh):
    return jax.shard_map(
        local,
        mesh=mesh,
        in_specs=(P("band", None, None, "fft"), P(), P("band")),
        out_specs=P("band", "fft", None),
        check_vma=False,
    )
```

```python
import math

import jax
import jax.numpy as jnp
import numpy as np
from jax import lax
from jax.experimental import pallas as pl
from jax.experimental.pallas import tpu as pltpu
from jax.sharding import PartitionSpec as P

NC = 144
NF = 288
KZ = 72
NCOLS = KZ * KZ
LANES = 128
LAYERS = 2
FOLD_WAVES = 40
FOLD_POINTS = 80
MESH = pl.DeviceIdType.MESH


def product(pattern, operand_a, operand_b):
    return jnp.einsum(pattern, operand_a, operand_b, precision=lax.Precision.HIGH)


def round_up(size, unit):
    return -(-size // unit) * unit


def phase_tables():
    wave = np.arange(KZ) - KZ // 2
    angles = np.mod(np.arange(NC)[:, None] * wave[None, :], NC) * (2.0 * math.pi / NC)
    return np.cos(angles), np.sin(angles)


def interpolation_matrix():
    offsets = np.arange(NF)[:, None] - 2 * np.arange(NC)[None, :]
    waves = np.arange(1, NC // 2)
    angles = np.mod(offsets[:, :, None] * waves, NF) * (2.0 * math.pi / NF)
    return ((1.0 + 2.0 * np.sum(np.cos(angles), axis=2)) / NC).astype(np.float32)


def line_table(planes_padded):
    cos_t, sin_t = phase_tables()
    table = np.zeros((planes_padded, 2, 2, KZ), np.float32)
    table[:NC, 0, 0], table[:NC, 0, 1] = cos_t, -sin_t
    table[:NC, 1, 0], table[:NC, 1, 1] = sin_t, cos_t
    return table


def fold_tables():
    half = KZ // 2
    points = np.arange(NC // 2 + 1)
    waves = np.concatenate([np.arange(half), [half]])
    angles = np.mod(points[:, None] * waves[None, :], NC) * (2.0 * math.pi / NC)
    tables = []
    for values in (np.cos(angles), np.sin(angles)):
        table = np.zeros((FOLD_POINTS, FOLD_WAVES), np.float32)
        table[: NC // 2 + 1, : half + 1] = values
        high = table.astype(jnp.bfloat16)
        low = (table - high.astype(np.float32)).astype(jnp.bfloat16)
        tables.append(np.concatenate([high, high, low], axis=1))
    return np.stack(tables)


def wave_slots(index):
    half = KZ // 2
    return jnp.where(index >= half, index - half, jnp.where(index == 0, half, KZ - index))


def exchange_kernel(scope, src, dst, send_sem, recv_sem, local_sem):
    band_size, fft_size = lax.axis_size("band"), lax.axis_size("fft")
    band, fft = lax.axis_index("band"), lax.axis_index("fft")
    layer = band_size // LAYERS
    if scope == "all":
        total, me = band_size * fft_size, band * fft_size + fft
    elif scope == "layer":
        total, me = layer * fft_size, lax.rem(band, layer) * fft_size + fft
    else:
        total, me = LAYERS, band // layer

    def device_of(target):
        if scope == "all":
            return (target // fft_size, lax.rem(target, fft_size))
        if scope == "layer":
            return (band // layer * layer + target // fft_size, lax.rem(target, fft_size))
        return (target * layer + lax.rem(band, layer), fft)

    barrier = pltpu.get_barrier_semaphore()
    targets = []
    for step in range(1, total):
        target = lax.rem(me + step, total)
        targets.append((target, device_of(target)))
        pl.semaphore_signal(barrier, inc=1, device_id=targets[-1][1], device_id_type=MESH)
    own = pltpu.make_async_copy(src.at[me], dst.at[me], local_sem)
    own.start()
    pl.semaphore_wait(barrier, total - 1)
    copies = []
    for step in range(1, total):
        target, device = targets[step - 1]
        copy = pltpu.make_async_remote_copy(
            src_ref=src.at[target],
            dst_ref=dst.at[me],
            send_sem=send_sem.at[step],
            recv_sem=recv_sem.at[step],
            device_id=device,
            device_id_type=MESH,
        )
        copy.start()
        copies.append(copy)
    own.wait()
    for copy in copies:
        copy.wait()


def exchange(blocks, scope, collective_id):
    total = blocks.shape[0]
    return pl.pallas_call(
        lambda *refs: exchange_kernel(scope, *refs),
        out_shape=jax.ShapeDtypeStruct(blocks.shape, blocks.dtype),
        in_specs=[pl.BlockSpec(memory_space=pl.ANY)],
        out_specs=pl.BlockSpec(memory_space=pl.ANY),
        scratch_shapes=[
            pltpu.SemaphoreType.DMA((total,)),
            pltpu.SemaphoreType.DMA((total,)),
            pltpu.SemaphoreType.DMA,
        ],
        compiler_params=pltpu.CompilerParams(collective_id=collective_id, has_side_effects=True),
        name=f"exchange_{scope}",
    )(blocks)


def split_rows(data):
    high = data.astype(jnp.bfloat16).astype(jnp.float32)
    return jnp.concatenate([high, data - high, high], axis=0).astype(jnp.bfloat16)


def plane_kernel(cols, columns, index, table, pick, out, rows, box, half_re, half_im):
    parts, _, lanes, cols_padded = columns.shape
    for part in range(parts):
        def turn(block, carry):
            at = pl.multiple_of(block * LANES, LANES)
            for which in range(2):
                rows[pl.ds(part * cols_padded + at, LANES), pl.ds(which * lanes, lanes)] = columns[
                    part, which, :, pl.ds(at, LANES)
                ].T
            return carry

        lax.fori_loop(0, cols_padded // LANES, turn, 0)

    unroll = math.gcd(cols, 16)
    for part in range(parts):
        def place(step, carry):
            first = step * unroll
            batch = [rows[pl.ds(part * cols_padded + first + n, 1), :] for n in range(unroll)]
            to = [index[part * cols + first + n] for n in range(unroll)]
            for row, value in zip(to, batch):
                box[pl.ds(row, 1), :] = value
            return carry

        lax.fori_loop(0, cols // unroll, place, 0)

    half = KZ // 2
    single = lax.broadcasted_iota(jnp.int32, (half + 4, 2 * lanes), 0)[:half] == 0
    last_row = lax.broadcasted_iota(jnp.int32, (8, 2 * lanes), 0)[: FOLD_WAVES - half] == 0

    def rotate(ahead, behind):
        alone = jnp.where(last_row, jnp.broadcast_to(behind[:1], last_row.shape), 0.0)
        behind = jnp.where(single, 0.0, behind)
        even = jnp.concatenate([ahead + behind, alone], axis=0)
        odd = jnp.concatenate([ahead - behind, -alone], axis=0)
        cos_part = jnp.dot(table[0], split_rows(even), preferred_element_type=jnp.float32)
        sin_part = jnp.dot(table[1], split_rows(odd), preferred_element_type=jnp.float32)
        cos_re, cos_im = cos_part[:, :lanes], cos_part[:, lanes:]
        sin_re, sin_im = sin_part[:, :lanes], sin_part[:, lanes:]
        real = jnp.concatenate([cos_re - sin_im, cos_re + sin_im], axis=0)
        imag = jnp.concatenate([cos_im + sin_re, cos_im - sin_re], axis=0)
        return real, imag

    slots = 2 * FOLD_POINTS

    def second(first, carry):
        at = pl.multiple_of(first * KZ, 8)
        data = box[pl.ds(at, KZ), :]
        real, imag = rotate(data[:half], data[half:])
        at = pl.ds(pl.multiple_of(first * slots, 8), slots)
        half_re[at, :] = real
        half_im[at, :] = imag
        return carry

    lax.fori_loop(0, KZ, second, 0, unroll=4)

    def third(point, carry):
        slot = jnp.where(point <= NC // 2, point, point + FOLD_POINTS - NC // 2)
        parts = []
        for base in (0, half):
            at = pl.ds(slot + base * slots, half, stride=slots)
            parts.append(jnp.concatenate([half_re[at, :], half_im[at, :]], axis=1))
        real, imag = rotate(*parts)
        moduli = real * real + imag * imag
        high = moduli.astype(jnp.bfloat16)
        low = (moduli - high.astype(jnp.float32)).astype(jnp.bfloat16)
        both = jnp.concatenate([high, low], axis=1)
        out[point] = lax.dot_general(
            pick[...], both, (((1,), (1,)), ((), ())), preferred_element_type=jnp.float32
        )
        return carry

    lax.fori_loop(0, NC, third, 0, unroll=4)


def local(coefficients, col_index, occupation):
    band_here, _, _, cols = coefficients.shape
    band_size, fft_size = lax.axis_size("band"), lax.axis_size("fft")
    total = band_size * fft_size
    bands = band_here * band_size
    layer = band_size // LAYERS
    group = layer * fft_size
    planes = -(-NC // group)
    radius = KZ // 2
    local_cols = lax.dynamic_slice_in_dim(col_index, lax.axis_index("fft") * cols, cols)
    first_wave = local_cols // KZ - radius
    second_wave = local_cols % KZ - radius
    third_wave = jnp.arange(KZ, dtype=jnp.int32) - radius
    radial = (first_wave * first_wave + second_wave * second_wave)[None, :] + (
        third_wave * third_wave
    )[:, None]
    inside = (radial <= radius * radius).astype(jnp.float32)
    amplitude = jnp.sqrt(occupation.astype(jnp.float32) / bands)
    masked = coefficients * inside * amplitude[:, None, None, None]

    table = jnp.asarray(line_table(group * planes))
    lines = product("zpqk,bqkc->zbpc", table, masked)
    lines = lines.reshape(group, planes * band_here, 2, cols)
    lines = exchange(lines, "layer", 0)

    columns = lines.reshape(layer, fft_size, planes * band_here, 2, cols)
    columns = columns.transpose(1, 3, 0, 2, 4).reshape(fft_size, 2, layer * planes * band_here, cols)
    lane_count = layer * planes * band_here
    lanes = round_up(lane_count, LANES)
    cols_padded = round_up(cols, LANES)
    columns = jnp.pad(columns, ((0, 0), (0, 0), (0, lanes - lane_count), (0, cols_padded - cols)))

    plane_rows = round_up(planes, 8)
    pick = np.zeros((plane_rows, lanes), np.float32)
    lane = np.arange(lane_count)
    pick[(lane // band_here) % planes, lane] = 1.0
    pick = jnp.asarray(np.concatenate([pick, pick], axis=1), jnp.bfloat16)

    places = wave_slots(col_index // KZ) * KZ + wave_slots(col_index % KZ)
    vmem = pl.BlockSpec(memory_space=pltpu.VMEM)
    density = pl.pallas_call(
        lambda *refs: plane_kernel(cols, *refs),
        out_shape=jax.ShapeDtypeStruct((NC, plane_rows, 2 * FOLD_POINTS), jnp.float32),
        in_specs=[vmem, pl.BlockSpec(memory_space=pltpu.SMEM), vmem, vmem],
        out_specs=vmem,
        scratch_shapes=[
            pltpu.VMEM((fft_size * cols_padded, 2 * lanes), jnp.float32),
            pltpu.VMEM((NCOLS, 2 * lanes), jnp.float32),
            pltpu.VMEM((KZ * 2 * FOLD_POINTS, lanes), jnp.float32),
            pltpu.VMEM((KZ * 2 * FOLD_POINTS, lanes), jnp.float32),
        ],
        compiler_params=pltpu.CompilerParams(vmem_limit_bytes=56 * 1024 * 1024),
        name="planes",
    )(columns, places, jnp.asarray(fold_tables()), pick)

    row_share = NF // band_size
    kept = NC // 2 + 1
    density = density[:, :planes]
    density = jnp.concatenate(
        [density[..., :kept], density[..., FOLD_POINTS + 1 : FOLD_POINTS + 1 + NC - kept]], axis=2
    )
    points = NC // LAYERS

    def exchange_flat(blocks, chunk, scope, collective_id):
        padded = round_up(chunk, LANES)
        flat = jnp.pad(blocks.reshape(-1, chunk), ((0, 0), (0, padded - chunk)))
        flat = flat.reshape(-1, padded // LANES, LANES)
        if scope == "all":
            flat = jnp.broadcast_to(flat[:, None], (band_size, fft_size) + flat.shape[1:])
            flat = flat.reshape((total,) + flat.shape[2:])
        return exchange(flat, scope, collective_id)

    part = exchange_flat(density, points * planes * NC, "column", 1)
    summed = jnp.sum(part, axis=0).reshape(-1)[: points * planes * NC]
    summed = summed.reshape(points, planes, NC)

    order = np.concatenate([np.arange(kept), np.arange(NC - 1, kept - 1, -1)])
    interpolation = jnp.asarray(interpolation_matrix()[:, order])
    row_share = NF // band_size
    wide = product("ga,pza->gzp", interpolation, summed)
    chunk = row_share * planes * points
    wide = exchange_flat(wide, chunk, "all", 2)
    wide = wide.reshape(total, -1)[:, :chunk].reshape(LAYERS, group, row_share, planes, points)

    col_share = NF // fft_size
    own = lax.dynamic_slice_in_dim(interpolation, lax.axis_index("fft") * col_share, col_share, 0)
    full = 0.0
    for half in range(LAYERS):
        own_half = own[:, half * points : (half + 1) * points]
        full = full + product("tgzb,fb->gftz", wide[half], own_half)
    full = full.reshape(row_share, col_share, group * planes)
    last = jnp.asarray(np.pad(interpolation_matrix(), ((0, 0), (0, group * planes - NC))))
    return product("gfz,hz->gfh", full, last)


def solution(mesh):
    return jax.shard_map(
        local,
        mesh=mesh,
        in_specs=(P("band", None, None, "fft"), P(), P("band")),
        out_specs=P("band", "fft", None),
        check_vma=False,
    )
```

```python
import math

import jax
import jax.numpy as jnp
import numpy as np
from jax import lax
from jax.experimental import pallas as pl
from jax.experimental.pallas import tpu as pltpu
from jax.sharding import PartitionSpec as P

NC = 144
NF = 288
KZ = 72
NCOLS = KZ * KZ
LANES = 128
LAYERS = 2
FOLD_WAVES = 40
FOLD_POINTS = 80
MESH = pl.DeviceIdType.MESH


def product(pattern, operand_a, operand_b):
    return jnp.einsum(pattern, operand_a, operand_b, precision=lax.Precision.HIGH)


def round_up(size, unit):
    return -(-size // unit) * unit


def phase_tables():
    wave = np.arange(KZ) - KZ // 2
    angles = np.mod(np.arange(NC)[:, None] * wave[None, :], NC) * (2.0 * math.pi / NC)
    return np.cos(angles), np.sin(angles)


def interpolation_matrix():
    offsets = np.arange(NF)[:, None] - 2 * np.arange(NC)[None, :]
    waves = np.arange(1, NC // 2)
    angles = np.mod(offsets[:, :, None] * waves, NF) * (2.0 * math.pi / NF)
    return ((1.0 + 2.0 * np.sum(np.cos(angles), axis=2)) / NC).astype(np.float32)


def line_table(planes_padded):
    cos_t, sin_t = phase_tables()
    table = np.zeros((planes_padded, 2, 2, KZ), np.float32)
    table[:NC, 0, 0], table[:NC, 0, 1] = cos_t, -sin_t
    table[:NC, 1, 0], table[:NC, 1, 1] = sin_t, cos_t
    return table


def fold_tables():
    half = KZ // 2
    points = np.arange(NC // 2 + 1)
    waves = np.concatenate([np.arange(half), [half]])
    angles = np.mod(points[:, None] * waves[None, :], NC) * (2.0 * math.pi / NC)
    tables = []
    for values in (np.cos(angles), np.sin(angles)):
        table = np.zeros((FOLD_POINTS, FOLD_WAVES), np.float32)
        table[: NC // 2 + 1, : half + 1] = values
        high = table.astype(jnp.bfloat16)
        low = (table - high.astype(np.float32)).astype(jnp.bfloat16)
        tables.append(np.concatenate([high, high, low], axis=1))
    return np.stack(tables)


def wave_slots(index):
    half = KZ // 2
    return jnp.where(index >= half, index - half, jnp.where(index == 0, half, KZ - index))


def exchange_kernel(scope, src, dst, send_sem, recv_sem, local_sem):
    band_size, fft_size = lax.axis_size("band"), lax.axis_size("fft")
    band, fft = lax.axis_index("band"), lax.axis_index("fft")
    layer = band_size // LAYERS
    if scope == "all":
        total, me = band_size * fft_size, band * fft_size + fft
    elif scope == "layer":
        total, me = layer * fft_size, lax.rem(band, layer) * fft_size + fft
    else:
        total, me = LAYERS, band // layer

    def device_of(target):
        if scope == "all":
            return (target // fft_size, lax.rem(target, fft_size))
        if scope == "layer":
            return (band // layer * layer + target // fft_size, lax.rem(target, fft_size))
        return (target * layer + lax.rem(band, layer), fft)

    barrier = pltpu.get_barrier_semaphore()
    targets = []
    for step in range(1, total):
        target = lax.rem(me + step, total)
        targets.append((target, device_of(target)))
        pl.semaphore_signal(barrier, inc=1, device_id=targets[-1][1], device_id_type=MESH)
    own = pltpu.make_async_copy(src.at[me], dst.at[me], local_sem)
    own.start()
    pl.semaphore_wait(barrier, total - 1)
    copies = []
    for step in range(1, total):
        target, device = targets[step - 1]
        copy = pltpu.make_async_remote_copy(
            src_ref=src.at[target],
            dst_ref=dst.at[me],
            send_sem=send_sem.at[step],
            recv_sem=recv_sem.at[step],
            device_id=device,
            device_id_type=MESH,
        )
        copy.start()
        copies.append(copy)
    own.wait()
    for copy in copies:
        copy.wait()


def exchange(blocks, scope, collective_id):
    total = blocks.shape[0]
    return pl.pallas_call(
        lambda *refs: exchange_kernel(scope, *refs),
        out_shape=jax.ShapeDtypeStruct(blocks.shape, blocks.dtype),
        in_specs=[pl.BlockSpec(memory_space=pl.ANY)],
        out_specs=pl.BlockSpec(memory_space=pl.ANY),
        scratch_shapes=[
            pltpu.SemaphoreType.DMA((total,)),
            pltpu.SemaphoreType.DMA((total,)),
            pltpu.SemaphoreType.DMA,
        ],
        compiler_params=pltpu.CompilerParams(collective_id=collective_id, has_side_effects=True),
        name=f"exchange_{scope}",
    )(blocks)


def split_rows(data):
    high = data.astype(jnp.bfloat16).astype(jnp.float32)
    return jnp.concatenate([high, data - high, high], axis=0).astype(jnp.bfloat16)


def plane_kernel(cols, columns, index, table, pick, out, rows, box, half_re, half_im):
    parts, _, lanes, cols_padded = columns.shape
    for part in range(parts):
        def turn(block, carry):
            at = pl.multiple_of(block * LANES, LANES)
            for which in range(2):
                rows[pl.ds(part * cols_padded + at, LANES), pl.ds(which * lanes, lanes)] = columns[
                    part, which, :, pl.ds(at, LANES)
                ].T
            return carry

        lax.fori_loop(0, cols_padded // LANES, turn, 0)

    unroll = math.gcd(cols, 16)
    for part in range(parts):
        def place(step, carry):
            first = step * unroll
            batch = [rows[pl.ds(part * cols_padded + first + n, 1), :] for n in range(unroll)]
            to = [index[part * cols + first + n] for n in range(unroll)]
            for row, value in zip(to, batch):
                box[pl.ds(row, 1), :] = value
            return carry

        lax.fori_loop(0, cols // unroll, place, 0)

    half = KZ // 2
    single = lax.broadcasted_iota(jnp.int32, (half + 4, 2 * lanes), 0)[:half] == 0
    last_row = lax.broadcasted_iota(jnp.int32, (8, 2 * lanes), 0)[: FOLD_WAVES - half] == 0

    def rotate(ahead, behind):
        alone = jnp.where(last_row, jnp.broadcast_to(behind[:1], last_row.shape), 0.0)
        behind = jnp.where(single, 0.0, behind)
        even = jnp.concatenate([ahead + behind, alone], axis=0)
        odd = jnp.concatenate([ahead - behind, -alone], axis=0)
        cos_part = jnp.dot(table[0], split_rows(even), preferred_element_type=jnp.float32)
        sin_part = jnp.dot(table[1], split_rows(odd), preferred_element_type=jnp.float32)
        cos_re, cos_im = cos_part[:, :lanes], cos_part[:, lanes:]
        sin_re, sin_im = sin_part[:, :lanes], sin_part[:, lanes:]
        real = jnp.concatenate([cos_re - sin_im, cos_re + sin_im], axis=0)
        imag = jnp.concatenate([cos_im + sin_re, cos_im - sin_re], axis=0)
        return real, imag

    slots = 2 * FOLD_POINTS

    def second(first, carry):
        at = pl.multiple_of(first * KZ, 8)
        data = box[pl.ds(at, KZ), :]
        real, imag = rotate(data[:half], data[half:])
        at = pl.ds(pl.multiple_of(first * slots, 8), slots)
        half_re[at, :] = real
        half_im[at, :] = imag
        return carry

    lax.fori_loop(0, KZ, second, 0, unroll=6)

    def third(point, carry):
        slot = jnp.where(point <= NC // 2, point, point + FOLD_POINTS - NC // 2)
        parts = []
        for base in (0, half):
            at = pl.ds(slot + base * slots, half, stride=slots)
            parts.append(jnp.concatenate([half_re[at, :], half_im[at, :]], axis=1))
        real, imag = rotate(*parts)
        moduli = real * real + imag * imag
        high = moduli.astype(jnp.bfloat16)
        low = (moduli - high.astype(jnp.float32)).astype(jnp.bfloat16)
        both = jnp.concatenate([high, low], axis=1)
        out[point] = lax.dot_general(
            pick[...], both, (((1,), (1,)), ((), ())), preferred_element_type=jnp.float32
        )
        return carry

    lax.fori_loop(0, NC, third, 0, unroll=6)


def local(coefficients, col_index, occupation):
    band_here, _, _, cols = coefficients.shape
    band_size, fft_size = lax.axis_size("band"), lax.axis_size("fft")
    total = band_size * fft_size
    bands = band_here * band_size
    layer = band_size // LAYERS
    group = layer * fft_size
    planes = -(-NC // group)
    radius = KZ // 2
    local_cols = lax.dynamic_slice_in_dim(col_index, lax.axis_index("fft") * cols, cols)
    first_wave = local_cols // KZ - radius
    second_wave = local_cols % KZ - radius
    third_wave = jnp.arange(KZ, dtype=jnp.int32) - radius
    radial = (first_wave * first_wave + second_wave * second_wave)[None, :] + (
        third_wave * third_wave
    )[:, None]
    inside = (radial <= radius * radius).astype(jnp.float32)
    amplitude = jnp.sqrt(occupation.astype(jnp.float32) / bands)
    masked = coefficients * inside * amplitude[:, None, None, None]

    table = jnp.asarray(line_table(group * planes))
    lines = product("zpqk,bqkc->zbpc", table, masked)
    lines = lines.reshape(group, planes * band_here, 2, cols)
    lines = exchange(lines, "layer", 0)

    columns = lines.reshape(layer, fft_size, planes * band_here, 2, cols)
    columns = columns.transpose(1, 3, 0, 2, 4).reshape(fft_size, 2, layer * planes * band_here, cols)
    lane_count = layer * planes * band_here
    lanes = round_up(lane_count, LANES)
    cols_padded = round_up(cols, LANES)
    columns = jnp.pad(columns, ((0, 0), (0, 0), (0, lanes - lane_count), (0, cols_padded - cols)))

    plane_rows = round_up(planes, 8)
    pick = np.zeros((plane_rows, lanes), np.float32)
    lane = np.arange(lane_count)
    pick[(lane // band_here) % planes, lane] = 1.0
    pick = jnp.asarray(np.concatenate([pick, pick], axis=1), jnp.bfloat16)

    places = wave_slots(col_index // KZ) * KZ + wave_slots(col_index % KZ)
    vmem = pl.BlockSpec(memory_space=pltpu.VMEM)
    density = pl.pallas_call(
        lambda *refs: plane_kernel(cols, *refs),
        out_shape=jax.ShapeDtypeStruct((NC, plane_rows, 2 * FOLD_POINTS), jnp.float32),
        in_specs=[vmem, pl.BlockSpec(memory_space=pltpu.SMEM), vmem, vmem],
        out_specs=vmem,
        scratch_shapes=[
            pltpu.VMEM((fft_size * cols_padded, 2 * lanes), jnp.float32),
            pltpu.VMEM((NCOLS, 2 * lanes), jnp.float32),
            pltpu.VMEM((KZ * 2 * FOLD_POINTS, lanes), jnp.float32),
            pltpu.VMEM((KZ * 2 * FOLD_POINTS, lanes), jnp.float32),
        ],
        compiler_params=pltpu.CompilerParams(vmem_limit_bytes=56 * 1024 * 1024),
        name="planes",
    )(columns, places, jnp.asarray(fold_tables()), pick)

    row_share = NF // band_size
    kept = NC // 2 + 1
    density = density[:, :planes]
    density = jnp.concatenate(
        [density[..., :kept], density[..., FOLD_POINTS + 1 : FOLD_POINTS + 1 + NC - kept]], axis=2
    )
    points = NC // LAYERS

    def exchange_flat(blocks, chunk, scope, collective_id):
        padded = round_up(chunk, LANES)
        flat = jnp.pad(blocks.reshape(-1, chunk), ((0, 0), (0, padded - chunk)))
        flat = flat.reshape(-1, padded // LANES, LANES)
        if scope == "all":
            flat = jnp.broadcast_to(flat[:, None], (band_size, fft_size) + flat.shape[1:])
            flat = flat.reshape((total,) + flat.shape[2:])
        return exchange(flat, scope, collective_id)

    part = exchange_flat(density, points * planes * NC, "column", 1)
    summed = jnp.sum(part, axis=0).reshape(-1)[: points * planes * NC]
    summed = summed.reshape(points, planes, NC)

    order = np.concatenate([np.arange(kept), np.arange(NC - 1, kept - 1, -1)])
    interpolation = jnp.asarray(interpolation_matrix()[:, order])
    row_share = NF // band_size
    wide = product("ga,pza->gzp", interpolation, summed)
    chunk = row_share * planes * points
    wide = exchange_flat(wide, chunk, "all", 2)
    wide = wide.reshape(total, -1)[:, :chunk].reshape(LAYERS, group, row_share, planes, points)

    col_share = NF // fft_size
    own = lax.dynamic_slice_in_dim(interpolation, lax.axis_index("fft") * col_share, col_share, 0)
    full = 0.0
    for half in range(LAYERS):
        own_half = own[:, half * points : (half + 1) * points]
        full = full + product("tgzb,fb->gftz", wide[half], own_half)
    full = full.reshape(row_share, col_share, group * planes)
    last = jnp.asarray(np.pad(interpolation_matrix(), ((0, 0), (0, group * planes - NC))))
    return product("gfz,hz->gfh", full, last)


def solution(mesh):
    return jax.shard_map(
        local,
        mesh=mesh,
        in_specs=(P("band", None, None, "fft"), P(), P("band")),
        out_specs=P("band", "fft", None),
        check_vma=False,
    )
```
